256 devices in a mesh: row: 32 (over z, y_hi, core), col: 8 (over x, y_lo).
Axes of the slice: x: 4, y: 4 (y_hi: 2, y_lo: 2; y = y_hi * 2 + y_lo), z: 8, core: 2. Of those that a mesh axis runs over, the one named last changes fastest.
Arguments:
- states: bfloat16 [768, 8192], P(None, 'col'), may hold values from -6 to 6
- norm_gain: float32 [8192], P('col'), may hold values from 0.25 to 1.75
- gate_weight: bfloat16 [8192, 28672], P('col', 'row'), may hold values from -0.0625 to 0.0625
- up_weight: bfloat16 [8192, 28672], P('col', 'row'), may hold values from -0.0625 to 0.0625
Outputs:
- near_tiles: float32 [32, 16, 896, 896], P('row', 'col')
- far_tiles: float32 [32, 896, 896], P('row', 'col')
The draws below stay inside these ranges and needn't reach their ends.
All inputs are finite; a program needn't handle non-finite values.
Results may differ from the reference program's by a relative error of at most 0.0071.
Values may be sent and summed in bfloat16 or wider, within the bound.
No kernel may reach another device: no remote copies, remote signals or barrier semaphores. Data moves between devices by JAX's collectives and lax.ppermute only.
A program may use at most 64 MiB of HBM per device.

```python
import jax
import jax.numpy as jnp
from jax import lax

D = 8192
FF = 28672
TOKENS = 768
BLOCK = 896
N_ROW = 32


def block_levels(stream_key, dims, cuts, smallest, high):
    factor_of = 1.0
    for dim, shards_of in cuts:
        draws = jax.random.uniform(jax.random.fold_in(jax.random.fold_in(stream_key, 6), dim), (shards_of,), jnp.float32, smallest / len(cuts), high / len(cuts))
        factor_of = factor_of * jnp.repeat(jnp.exp(draws), dims[dim] // shards_of).reshape((-1,) + (1,) * (len(dims) - 1 - dim))
    return factor_of


def noise(own_key, dims, spread, bound, split=(), kind=jnp.bfloat16):
    values = jax.random.normal(own_key, dims, jnp.float32) * spread
    if len(split) > 0:
        values = block_levels(own_key, dims, split, -0.22, 0.18) * values
    return jnp.clip(values, min=-bound, max=bound).astype(kind)


def setup_inputs(seed: int = 0) -> dict:
    arg_keys = jax.random.split(jax.random.key(seed), 5)
    states = noise(arg_keys[0], (TOKENS, D), 1.0, 6.0, ((1, 8),))
    norm_gain = jnp.clip(1.0 + 0.15 * jax.random.normal(arg_keys[1], (D,), jnp.float32), 0.25, 1.75)
    gate_weight = noise(arg_keys[2], (D, FF), D ** -0.5, 0.0625, ((0, 8), (1, 32)))
    up_weight = noise(arg_keys[3], (D, FF), D ** -0.5, 0.0625, ((0, 8), (1, 32)))
    return dict(states=states, norm_gain=norm_gain, gate_weight=gate_weight, up_weight=up_weight)


def reference(states, norm_gain, gate_weight, up_weight):
    wide = states.astype(jnp.float32)
    inverse = lax.rsqrt(lax.optimization_barrier(jnp.mean(wide * wide, axis=1)) + 1e-05)
    normed = (wide * inverse[:, None] * norm_gain[None, :]).astype(jnp.bfloat16)
    gate = jnp.dot(normed, gate_weight, preferred_element_type=jnp.float32)
    up = jnp.dot(normed, up_weight, preferred_element_type=jnp.float32)
    keys = (jax.nn.silu(gate) * up).astype(jnp.bfloat16)
    count = keys.shape[0]
    blocks = keys.astype(jnp.float32).reshape(count, N_ROW, BLOCK)
    half = N_ROW // 2

    def one_block(index):
        own = lax.dynamic_index_in_dim(blocks, index, 1, keepdims=False)
        rolled = jnp.roll(blocks, -index, axis=1)
        near = jnp.einsum('tk,tmj->mkj', own, rolled[:, :half], precision=lax.Precision.HIGHEST) / count
        far = jnp.einsum('tk,tj->kj', own, rolled[:, half], precision=lax.Precision.HIGHEST) / count
        return (near, far)
    near_tiles, far_tiles = lax.map(one_block, jnp.arange(N_ROW, dtype=jnp.int32))
    return (near_tiles, far_tiles)
```

```python
import jax
import jax.numpy as jnp
from jax import lax
from jax.sharding import Mesh
from jax.sharding import PartitionSpec as P

D = 8192
ROW = ("z", "yh", "k")
COL = ("x", "yl")
PLANE = ("x", "yh", "yl")


def exchange(pieces, axes):
    return lax.all_to_all(pieces, axes, split_axis=0, concat_axis=0, tiled=True)


def copy_for_each(shard, axes):
    return exchange(jnp.broadcast_to(shard, (lax.axis_size(axes), *shard.shape)), axes)


def passed_along(shard, axis, by):
    devices = lax.axis_size(axis)
    return lax.ppermute(shard, axis, [(i, (i + by) % devices) for i in range(devices)])


def cross(left, right):
    return lax.dot_general(
        left, right, (((0,), (0,)), ((), ())), preferred_element_type=jnp.float32
    )


def on_device(states, norm_gain, gate_weight, up_weight):
    n_col = lax.axis_size(COL)
    column = lax.axis_index(COL)
    yh, yl, core = lax.axis_index("yh"), lax.axis_index("yl"), lax.axis_index("k")
    count = states.shape[0]
    width = gate_weight.shape[1]
    share = count // n_col
    scale = 1.0 / count

    wide = states.astype(jnp.float32)
    squares = jnp.sum(copy_for_each(jnp.sum(wide * wide, axis=1), COL), axis=0)
    inverse = lax.rsqrt(squares / D + 1e-05)
    normed = (wide * inverse[:, None] * norm_gain[None, :]).astype(jnp.bfloat16)
    gate_part = jnp.dot(normed, gate_weight, preferred_element_type=jnp.float32)
    up_part = jnp.dot(normed, up_weight, preferred_element_type=jnp.float32)
    parts = jnp.concatenate(
        [gate_part.astype(jnp.bfloat16), up_part.astype(jnp.bfloat16)], axis=1
    )
    parts = exchange(parts.reshape(n_col, share, 2 * width), COL)
    summed = jnp.sum(parts.astype(jnp.float32), axis=0)
    own = (jax.nn.silu(summed[:, :width]) * summed[:, width:]).astype(jnp.bfloat16)

    keys = copy_for_each(own, COL).reshape(count, width)

    ahead = [own]
    for _ in range(4):
        ahead.append(passed_along(ahead[-1], "z", -1))
    mixed = [jnp.where(yh == 0, ahead[j + 1], ahead[j]) for j in range(4)]
    outgoing = []
    for j in range(4):
        outgoing += [ahead[j], mixed[j], mixed[j], ahead[j + 1]]
    outgoing, keys = lax.optimization_barrier((jnp.stack(outgoing, axis=0), keys))
    returned = exchange(outgoing, PLANE)
    slab = width // n_col
    own_cols = lax.dynamic_slice_in_dim(keys, column * slab, slab, 1)
    their_cols = passed_along(own_cols, "z", 4)
    their_far = (cross(their_cols, keys) * scale).astype(jnp.bfloat16)
    far_rows = passed_along(their_far, "z", 4)
    returned, far_rows = lax.optimization_barrier((returned, far_rows))
    far_tiles = far_rows.astype(jnp.float32)[None]

    returned = returned.reshape(4, 2, 2, share, width)
    near = jnp.bitwise_xor(yh, yl)
    first = lax.dynamic_index_in_dim(returned, near, 1, keepdims=False)
    swap = jnp.where(core == 0, 1 - near, near)
    second = lax.dynamic_index_in_dim(returned, swap, 1, keepdims=False)
    second = passed_along(second, "k", 1)

    tiles = [
        cross(keys, partner.reshape(count, width)) * scale for partner in (first, second)
    ]
    near_tiles = jnp.stack(tiles, axis=0)[None]
    return (near_tiles, far_tiles)


def solution(mesh):
    torus = Mesh(mesh.devices.reshape(8, 2, 2, 4, 2), ("z", "yh", "k", "x", "yl"))
    in_specs = (P(None, COL), P(COL), P(COL, ROW), P(COL, ROW))
    out_specs = (P(ROW, COL, None, None), P(ROW, COL, None))
    return jax.shard_map(
        on_device, mesh=torus, in_specs=in_specs, out_specs=out_specs, check_vma=False
    )
```

```python
import jax
import jax.numpy as jnp
from jax import lax
from jax.experimental import pallas as pl
from jax.experimental.pallas import tpu as pltpu
from jax.sharding import Mesh
from jax.sharding import PartitionSpec as P

D = 8192
ROW = ("z", "yh", "k")
COL = ("x", "yl")
PLANE = ("x", "yh", "yl")


def exchange(pieces, axes):
    return lax.all_to_all(pieces, axes, split_axis=0, concat_axis=0, tiled=True)


def copy_for_each(shard, axes):
    return exchange(jnp.broadcast_to(shard, (lax.axis_size(axes), *shard.shape)), axes)


def passed_along(shard, axis, by):
    devices = lax.axis_size(axis)
    return lax.ppermute(shard, axis, [(i, (i + by) % devices) for i in range(devices)])


def cross(left, right):
    return lax.dot_general(
        left, right, (((0,), (0,)), ((), ())), preferred_element_type=jnp.float32
    )


def tile_kernel(pick_ref, left_ref, right_ref, *refs):
    out_ref = refs[-1]
    right = right_ref[...]
    right = right.reshape(-1, right.shape[-1])
    product = jnp.dot(left_ref[...], right, preferred_element_type=jnp.float32)
    out_ref[...] = (product * (1.0 / right.shape[0]))[None]


def tile_into(place, keys_t, pieces, pick, tiles=None, steps=2):
    width, count = keys_t.shape
    groups, _, parts, share, _ = pieces.shape
    rows = width // steps
    in_specs = [
        pl.BlockSpec((rows, count), lambda i, p: (i, 0)),
        pl.BlockSpec((groups, 1, parts, share, width), lambda i, p: (0, p[0], 0, 0, 0)),
    ]
    args = [keys_t, pieces]
    aliases = {}
    if tiles is not None:
        in_specs.append(pl.BlockSpec(memory_space=pl.ANY))
        args.append(tiles)
        aliases = {3: 0}
    return pl.pallas_call(
        tile_kernel,
        grid_spec=pltpu.PrefetchScalarGridSpec(
            num_scalar_prefetch=1,
            grid=(steps,),
            in_specs=in_specs,
            out_specs=pl.BlockSpec((1, rows, width), lambda i, p: (place, i, 0)),
        ),
        out_shape=jax.ShapeDtypeStruct((2, width, width), jnp.float32),
        input_output_aliases=aliases,
        cost_estimate=pl.CostEstimate(
            flops=2 * width * width * count,
            bytes_accessed=4 * width * count + 4 * width * width,
            transcendentals=0,
        ),
        name="tile",
    )(pick.reshape(1), *args)


def on_device(states, norm_gain, gate_weight, up_weight):
    n_col = lax.axis_size(COL)
    column = lax.axis_index(COL)
    yh, yl, core = lax.axis_index("yh"), lax.axis_index("yl"), lax.axis_index("k")
    count = states.shape[0]
    width = gate_weight.shape[1]
    share = count // n_col
    half = count // 2
    scale = 1.0 / count

    squares = jnp.sum(jnp.square(states.astype(jnp.float32)), axis=1)
    squares = jnp.sum(copy_for_each(squares, COL), axis=0)
    inverse = lax.rsqrt(squares / D + 1e-05)

    def partial_sums(tokens, factor):
        normed = tokens.astype(jnp.float32) * factor[:, None] * norm_gain[None, :]
        normed = normed.astype(jnp.bfloat16)
        parts = [
            jnp.dot(normed, weight, preferred_element_type=jnp.float32).astype(jnp.bfloat16)
            for weight in (gate_weight, up_weight)
        ]
        return jnp.concatenate(parts, axis=1).reshape(n_col, share // 2, 2 * width)

    def keys_of(parts):
        summed = jnp.sum(parts.astype(jnp.float32), axis=0)
        return (jax.nn.silu(summed[:, :width]) * summed[:, width:]).astype(jnp.bfloat16)

    def along_z(keys):
        return [keys] + [passed_along(keys, "z", by) for by in (-1, -2, -3, -4)]

    one = partial_sums(states[:half], inverse[:half])
    two = partial_sums(states[half:], inverse[half:])
    one = exchange(one, COL)
    one, two = lax.optimization_barrier((one, two))
    two = exchange(two, COL)
    own_one = keys_of(one)
    ahead_one = along_z(own_one)
    two, ahead_one = lax.optimization_barrier((two, ahead_one))
    own_two = keys_of(two)

    keys = copy_for_each(jnp.concatenate([own_one, own_two], axis=0), COL)
    keys = keys.reshape(count, width)
    ahead_two = along_z(own_two)

    outgoing = []
    for j in range(4):
        here = [ahead_one[j], ahead_two[j]]
        after = [ahead_one[j + 1], ahead_two[j + 1]]
        mixed = [jnp.where(yh == 0, b, a) for a, b in zip(here, after)]
        outgoing += here + mixed + mixed + after
    outgoing = jnp.concatenate(outgoing, axis=0).reshape(16, share, width)
    outgoing, keys = lax.optimization_barrier((outgoing, keys))
    returned = exchange(outgoing, PLANE)

    slab = width // n_col
    own_cols = lax.dynamic_slice_in_dim(keys, column * slab, slab, 1)
    their_cols = passed_along(own_cols, "z", 4)
    their_far = (cross(their_cols, keys) * scale).astype(jnp.bfloat16)
    far_tiles = passed_along(their_far, "z", 4).astype(jnp.float32)[None]
    keys_t = keys.T
    returned, far_tiles, keys_t = lax.optimization_barrier((returned, far_tiles, keys_t))

    returned = returned.reshape(4, 2, 2, share, width)
    near = jnp.bitwise_xor(yh, yl)
    swap = jnp.where(core == 0, 1 - near, near)
    second = lax.dynamic_slice_in_dim(returned, swap, 1, 1)
    second = passed_along(second, "k", 1)
    tiles = tile_into(0, keys_t, returned, near)
    tiles = tile_into(1, keys_t, second, jnp.zeros_like(near), tiles)
    return (tiles[None], far_tiles)


def solution(mesh):
    torus = Mesh(mesh.devices.reshape(8, 2, 2, 4, 2), ("z", "yh", "k", "x", "yl"))
    in_specs = (P(None, COL), P(COL), P(COL, ROW), P(COL, ROW))
    out_specs = (P(ROW, COL, None, None), P(ROW, COL, None))
    return jax.shard_map(
        on_device, mesh=torus, in_specs=in_specs, out_specs=out_specs, check_vma=False
    )
```

```python
import functools

import jax
import jax.numpy as jnp
from jax import lax
from jax.experimental import pallas as pl
from jax.experimental.pallas import tpu as pltpu
from jax.sharding import Mesh
from jax.sharding import PartitionSpec as P

D = 8192
ROW = ("z", "yh", "k")
COL = ("x", "yl")
PLANE = ("x", "yh", "yl")
SLOTS_VMEM = 4 * 2**20
TILE_VMEM = 16 * 2**20


def exchange(pieces, axes):
    return lax.all_to_all(pieces, axes, split_axis=0, concat_axis=0, tiled=True)


def copy_for_each(shard, axes):
    return exchange(jnp.broadcast_to(shard, (lax.axis_size(axes), *shard.shape)), axes)


def passed_along(shard, axis, by):
    devices = lax.axis_size(axis)
    return lax.ppermute(shard, axis, [(i, (i + by) % devices) for i in range(devices)])


def cross(left, right):
    return lax.dot_general(
        left, right, (((0,), (0,)), ((), ())), preferred_element_type=jnp.float32
    )


def slots_kernel(*refs):
    ahead, out_ref, sems = refs[:5], refs[5], refs[6]
    yh = lax.axis_index("yh")

    def copy(j, slot):
        return pltpu.make_async_copy(ahead[j], out_ref.at[slot], sems.at[slot])

    for j in range(4):
        copy(j, 4 * j).start()
        copy(j + 1, 4 * j + 3).start()
        for slot in (4 * j + 1, 4 * j + 2):

            @pl.when(yh == 0)
            def _():
                copy(j + 1, slot).start()

            @pl.when(yh != 0)
            def _():
                copy(j, slot).start()

    for slot in range(16):
        copy(0, slot).wait()


def slots(ahead):
    return pl.pallas_call(
        slots_kernel,
        in_specs=[pl.BlockSpec(memory_space=pltpu.VMEM)] * 5,
        out_specs=pl.BlockSpec(memory_space=pltpu.HBM),
        out_shape=pltpu.HBM((16, *ahead[0].shape), ahead[0].dtype),
        scratch_shapes=[pltpu.SemaphoreType.DMA((16,))],
        cost_estimate=pl.CostEstimate(
            flops=16 * ahead[0].size, bytes_accessed=42 * ahead[0].size, transcendentals=0
        ),
        compiler_params=pltpu.CompilerParams(vmem_limit_bytes=SLOTS_VMEM),
        name="slots",
    )(*ahead)


def tile_kernel(place, left_ref, right_ref, *refs):
    out_ref, rows_ref, sems = refs[-3:]
    chunks, rows, _ = rows_ref.shape
    scale = 1.0 / right_ref.shape[0]

    def copy(i):
        return pltpu.make_async_copy(
            rows_ref.at[i], out_ref.at[place, pl.ds(i * rows, rows)], sems.at[i]
        )

    for i in range(chunks):
        left = left_ref[i * rows : (i + 1) * rows, :]
        product = jnp.dot(left, right_ref[...], preferred_element_type=jnp.float32)
        rows_ref[i] = product * scale
        copy(i).start()
    for i in range(chunks):
        copy(i).wait()


def tile_into(place, keys_t, partner, tiles=None, chunks=4):
    width, count = keys_t.shape
    rows = width // chunks
    in_specs = [pl.BlockSpec(memory_space=pltpu.VMEM)] * 2
    args = [keys_t, partner]
    if tiles is not None:
        in_specs.append(pl.BlockSpec(memory_space=pltpu.HBM))
        args.append(tiles)
    return pl.pallas_call(
        functools.partial(tile_kernel, place),
        in_specs=in_specs,
        out_specs=pl.BlockSpec(memory_space=pltpu.HBM),
        out_shape=pltpu.HBM((2, width, width), jnp.float32),
        scratch_shapes=[
            pltpu.VMEM((chunks, rows, width), jnp.float32),
            pltpu.SemaphoreType.DMA((chunks,)),
        ],
        input_output_aliases={} if tiles is None else {2: 0},
        cost_estimate=pl.CostEstimate(
            flops=2 * width * width * count,
            bytes_accessed=4 * width * count + 4 * width * width,
            transcendentals=0,
        ),
        compiler_params=pltpu.CompilerParams(vmem_limit_bytes=TILE_VMEM),
        name="tile",
    )(*args)


def on_device(states, norm_gain, gate_weight, up_weight):
    n_col = lax.axis_size(COL)
    column = lax.axis_index(COL)
    yh, yl, core = lax.axis_index("yh"), lax.axis_index("yl"), lax.axis_index("k")
    count = states.shape[0]
    width = gate_weight.shape[1]
    share = count // n_col
    scale = 1.0 / count

    wide = states.astype(jnp.float32)
    squares = jnp.sum(copy_for_each(jnp.sum(wide * wide, axis=1), COL), axis=0)
    inverse = lax.rsqrt(squares / D + 1e-05)
    normed = (wide * inverse[:, None] * norm_gain[None, :]).astype(jnp.bfloat16)
    gate_part = jnp.dot(normed, gate_weight, preferred_element_type=jnp.float32)
    up_part = jnp.dot(normed, up_weight, preferred_element_type=jnp.float32)
    parts = jnp.concatenate(
        [gate_part.astype(jnp.bfloat16), up_part.astype(jnp.bfloat16)], axis=1
    )
    parts = exchange(parts.reshape(n_col, share, 2 * width), COL)
    summed = jnp.sum(parts.astype(jnp.float32), axis=0)
    own = (jax.nn.silu(summed[:, :width]) * summed[:, width:]).astype(jnp.bfloat16)

    ahead = [own]
    two = passed_along(own, "z", -2)
    own_late = own
    one = passed_along(two, "z", 1)
    three = passed_along(two, "z", -1)
    keys = copy_for_each(own_late, COL).reshape(count, width)
    ahead = [own, one, two, three, passed_along(three, "z", -1)]
    outgoing, keys = lax.optimization_barrier((slots(ahead), keys))
    returned = exchange(outgoing, PLANE)

    slab = width // n_col
    own_cols = lax.dynamic_slice_in_dim(keys, column * slab, slab, 1)
    their_cols = passed_along(own_cols, "z", 4)
    their_far = (cross(their_cols, keys) * scale).astype(jnp.bfloat16)
    far_tiles = passed_along(their_far, "z", 4).astype(jnp.float32)[None]
    returned, far_tiles, keys_t = lax.optimization_barrier((returned, far_tiles, keys.T))

    returned = returned.reshape(4, 2, 2, share, width)
    near = jnp.bitwise_xor(yh, yl)
    swap = jnp.where(core == 0, 1 - near, near)
    second = lax.dynamic_index_in_dim(returned, swap, 1, keepdims=False)
    second = passed_along(second.reshape(count, width), "k", 1)
    first = lax.dynamic_index_in_dim(returned, near, 1, keepdims=False)
    tiles = tile_into(0, keys_t, first.reshape(count, width))
    near_tiles = tile_into(1, keys_t, second, tiles)[None]
    return (near_tiles, far_tiles)


def solution(mesh):
    torus = Mesh(mesh.devices.reshape(8, 2, 2, 4, 2), ("z", "yh", "k", "x", "yl"))
    in_specs = (P(None, COL), P(COL), P(COL, ROW), P(COL, ROW))
    out_specs = (P(ROW, COL, None, None), P(ROW, COL, None))
    return jax.shard_map(
        on_device, mesh=torus, in_specs=in_specs, out_specs=out_specs, check_vma=False
    )
```

```python
import functools

import jax
import jax.numpy as jnp
from jax import lax
from jax.experimental import pallas as pl
from jax.experimental.pallas import tpu as pltpu
from jax.sharding import Mesh
from jax.sharding import PartitionSpec as P


D = 8192
ROW = ("z", "yh", "k")
COL = ("x", "yl")
PLANE = ("x", "yh", "yl")
SLOTS_VMEM = 4 * 2**20
TILE_VMEM = 16 * 2**20


def exchange(pieces, axes):
    return lax.all_to_all(pieces, axes, split_axis=0, concat_axis=0, tiled=True)


def copy_for_each(shard, axes):
    return exchange(jnp.broadcast_to(shard, (lax.axis_size(axes), *shard.shape)), axes)


def passed_along(shard, axis, by):
    devices = lax.axis_size(axis)
    return lax.ppermute(shard, axis, [(i, (i + by) % devices) for i in range(devices)])


def cross(left, right):
    return lax.dot_general(
        left, right, (((0,), (0,)), ((), ())), preferred_element_type=jnp.float32
    )


def slots_kernel(*refs):
    ahead, out_ref, sems = refs[:5], refs[5], refs[6]
    yh = lax.axis_index("yh")

    def copy(j, slot):
        return pltpu.make_async_copy(ahead[j], out_ref.at[slot], sems.at[slot])

    for j in range(4):
        copy(j, 4 * j).start()
        copy(j + 1, 4 * j + 3).start()
        for slot in (4 * j + 1, 4 * j + 2):

            @pl.when(yh == 0)
            def _():
                copy(j + 1, slot).start()

            @pl.when(yh != 0)
            def _():
                copy(j, slot).start()

    for slot in range(16):
        copy(0, slot).wait()


def slots(ahead):
    return pl.pallas_call(
        slots_kernel,
        in_specs=[pl.BlockSpec(memory_space=pltpu.VMEM)] * 5,
        out_specs=pl.BlockSpec(memory_space=pltpu.HBM),
        out_shape=pltpu.HBM((16, *ahead[0].shape), ahead[0].dtype),
        scratch_shapes=[pltpu.SemaphoreType.DMA((16,))],
        cost_estimate=pl.CostEstimate(
            flops=16 * ahead[0].size, bytes_accessed=42 * ahead[0].size, transcendentals=0
        ),
        compiler_params=pltpu.CompilerParams(vmem_limit_bytes=SLOTS_VMEM),
        name="slots",
    )(*ahead)


def tile_kernel(place, left_ref, right_ref, *refs):
    out_ref, rows_ref, sems = refs[-3:]
    chunks, rows, _ = rows_ref.shape
    scale = 1.0 / right_ref.shape[0]

    def copy(i):
        return pltpu.make_async_copy(
            rows_ref.at[i], out_ref.at[place, pl.ds(i * rows, rows)], sems.at[i]
        )

    for i in range(chunks):
        left = left_ref[i * rows : (i + 1) * rows, :]
        product = jnp.dot(left, right_ref[...], preferred_element_type=jnp.float32)
        rows_ref[i] = product * scale
        copy(i).start()
    for i in range(chunks):
        copy(i).wait()


def tile_into(place, keys_t, partner, tiles=None, chunks=4):
    width, count = keys_t.shape
    rows = width // chunks
    in_specs = [pl.BlockSpec(memory_space=pltpu.VMEM)] * 2
    args = [keys_t, partner]
    if tiles is not None:
        in_specs.append(pl.BlockSpec(memory_space=pltpu.HBM))
        args.append(tiles)
    return pl.pallas_call(
        functools.partial(tile_kernel, place),
        in_specs=in_specs,
        out_specs=pl.BlockSpec(memory_space=pltpu.HBM),
        out_shape=pltpu.HBM((2, width, width), jnp.float32),
        scratch_shapes=[
            pltpu.VMEM((chunks, rows, width), jnp.float32),
            pltpu.SemaphoreType.DMA((chunks,)),
        ],
        input_output_aliases={} if tiles is None else {2: 0},
        cost_estimate=pl.CostEstimate(
            flops=2 * width * width * count,
            bytes_accessed=4 * width * count + 4 * width * width,
            transcendentals=0,
        ),
        compiler_params=pltpu.CompilerParams(vmem_limit_bytes=TILE_VMEM),
        name="tile",
    )(*args)


def fetch_kernel(states_in, gate_in, up_in, squares_ref, states_ref, gate_ref, up_ref, sems):
    pairs = ((states_in, states_ref), (gate_in, gate_ref), (up_in, up_ref))
    copies = [pltpu.make_async_copy(a, b, sems.at[i]) for i, (a, b) in enumerate(pairs)]
    for copy in copies:
        copy.start()
    copies[0].wait()
    wide = states_ref[...].astype(jnp.float32)
    total = jnp.sum(wide * wide, axis=1, keepdims=True)
    total = jnp.broadcast_to(total, (wide.shape[0], 128)).T
    squares_ref[...] = jnp.broadcast_to(total[None, :1], squares_ref.shape)
    for copy in copies[1:]:
        copy.wait()


def fetched(states, gate_weight, up_weight, copies):
    arrays = (states, gate_weight, up_weight)
    count, depth = states.shape
    return pl.pallas_call(
        fetch_kernel,
        in_specs=[pl.BlockSpec(memory_space=pltpu.HBM)] * 3,
        out_specs=[pl.BlockSpec(memory_space=pltpu.VMEM)] * 4,
        out_shape=[pltpu.VMEM((copies, 1, count), jnp.float32)]
        + [pltpu.VMEM(array.shape, array.dtype) for array in arrays],
        scratch_shapes=[pltpu.SemaphoreType.DMA((3,))],
        cost_estimate=pl.CostEstimate(
            flops=2 * count * depth,
            bytes_accessed=2 * sum(array.size for array in arrays),
            transcendentals=0,
        ),
        compiler_params=pltpu.CompilerParams(vmem_limit_bytes=58 * 2**20),
        name="fetch",
    )(*arrays)


def sums_kernel(states_ref, squares_ref, gain_ref, gate_ref, up_ref, out_ref):
    width = gate_ref.shape[1]
    squares = jnp.sum(squares_ref[...], axis=0)
    inverse = lax.rsqrt(squares / D + 1e-05)
    inverse = jnp.broadcast_to(inverse, (128, inverse.shape[1])).T[:, :1]
    rows = states_ref.shape[0] // 2
    for i in range(2):
        at = slice(i * rows, (i + 1) * rows)
        normed = states_ref[at, :].astype(jnp.float32) * inverse[at, :] * gain_ref[...]
        normed = normed.astype(jnp.bfloat16)
        for j, weight in enumerate((gate_ref, up_ref)):
            part = jnp.dot(normed, weight[...], preferred_element_type=jnp.float32)
            out_ref[at, j * width : (j + 1) * width] = part.astype(jnp.bfloat16)


def partial_sums(states, squares, norm_gain, gate_weight, up_weight):
    count, depth = states.shape
    width = gate_weight.shape[1]
    return pl.pallas_call(
        sums_kernel,
        in_specs=[pl.BlockSpec(memory_space=pltpu.VMEM)] * 5,
        out_specs=pl.BlockSpec(memory_space=pltpu.VMEM),
        out_shape=jax.ShapeDtypeStruct((count, 2 * width), jnp.bfloat16),
        cost_estimate=pl.CostEstimate(
            flops=4 * count * depth * width,
            bytes_accessed=2 * (count * depth + 2 * depth * width + 2 * count * width),
            transcendentals=0,
        ),
        compiler_params=pltpu.CompilerParams(vmem_limit_bytes=24 * 2**20),
        name="sums",
    )(states, squares, norm_gain[None, :], gate_weight, up_weight)


def on_device(states, norm_gain, gate_weight, up_weight):
    n_col = lax.axis_size(COL)
    column = lax.axis_index(COL)
    yh, yl, core = lax.axis_index("yh"), lax.axis_index("yl"), lax.axis_index("k")
    count = states.shape[0]
    width = gate_weight.shape[1]
    share = count // n_col
    scale = 1.0 / count

    squares, *arrays = fetched(states, gate_weight, up_weight, n_col)
    parts = partial_sums(arrays[0], exchange(squares, COL), norm_gain, *arrays[1:])
    parts = exchange(parts.reshape(n_col, share, 2 * width), COL)
    summed = jnp.sum(parts.astype(jnp.float32), axis=0)
    own = (jax.nn.silu(summed[:, :width]) * summed[:, width:]).astype(jnp.bfloat16)

    ahead = [own]
    two = passed_along(own, "z", -2)
    one = passed_along(two, "z", 1)
    three = passed_along(two, "z", -1)
    keys = copy_for_each(own, COL).reshape(count, width)
    ahead = [own, one, two, three, passed_along(three, "z", -1)]
    outgoing, keys = lax.optimization_barrier((slots(ahead), keys))
    returned = exchange(outgoing, PLANE)

    slab = width // n_col
    own_cols = lax.dynamic_slice_in_dim(keys, column * slab, slab, 1)
    their_cols = passed_along(own_cols, "z", 4)
    their_far = (cross(their_cols, keys) * scale).astype(jnp.bfloat16)
    far_tiles = passed_along(their_far, "z", 4).astype(jnp.float32)[None]
    returned, far_tiles, keys_t = lax.optimization_barrier((returned, far_tiles, keys.T))

    returned = returned.reshape(4, 2, 2, share, width)
    near = jnp.bitwise_xor(yh, yl)
    swap = jnp.where(core == 0, 1 - near, near)
    second = lax.dynamic_index_in_dim(returned, swap, 1, keepdims=False)
    second = passed_along(second.reshape(count, width), "k", 1)
    first = lax.dynamic_index_in_dim(returned, near, 1, keepdims=False)
    tiles = tile_into(0, keys_t, first.reshape(count, width))
    near_tiles = tile_into(1, keys_t, second, tiles)[None]
    return (near_tiles, far_tiles)


def solution(mesh):
    torus = Mesh(mesh.devices.reshape(8, 2, 2, 4, 2), ("z", "yh", "k", "x", "yl"))
    in_specs = (P(None, COL), P(COL), P(COL, ROW), P(COL, ROW))
    out_specs = (P(ROW, COL, None, None), P(ROW, COL, None))

    return jax.shard_map(
        on_device, mesh=torus, in_specs=in_specs, out_specs=out_specs, check_vma=False
    )
```

```python
import functools

import jax
import jax.numpy as jnp
from jax import lax
from jax.experimental import pallas as pl
from jax.experimental.pallas import tpu as pltpu
from jax.sharding import Mesh
from jax.sharding import PartitionSpec as P


D = 8192
ROW = ("z", "yh", "k")
COL = ("x", "yl")
PLANE = ("x", "yh", "yl")
SLOTS_VMEM = 4 * 2**20
TILE_VMEM = 16 * 2**20
PIECES = ((0, 448), (448, 256), (704, 128), (832, 64))


def exchange(pieces, axes):
    return lax.all_to_all(pieces, axes, split_axis=0, concat_axis=0, tiled=True)


def copy_for_each(shard, axes):
    return exchange(jnp.broadcast_to(shard, (lax.axis_size(axes), *shard.shape)), axes)


def passed_along(shard, axis, by):
    devices = lax.axis_size(axis)
    return lax.ppermute(shard, axis, [(i, (i + by) % devices) for i in range(devices)])


def cross(left, right):
    return lax.dot_general(
        left, right, (((0,), (0,)), ((), ())), preferred_element_type=jnp.float32
    )


def slots_kernel(*refs):
    ahead, out_ref, sems = refs[:5], refs[5], refs[6]
    yh = lax.axis_index("yh")

    def copy(j, slot):
        return pltpu.make_async_copy(ahead[j], out_ref.at[slot], sems.at[slot])

    for j in range(4):
        copy(j, 4 * j).start()
        copy(j + 1, 4 * j + 3).start()
        for slot in (4 * j + 1, 4 * j + 2):

            @pl.when(yh == 0)
            def _():
                copy(j + 1, slot).start()

            @pl.when(yh != 0)
            def _():
                copy(j, slot).start()

    for slot in range(16):
        copy(0, slot).wait()


def slots(ahead):
    return pl.pallas_call(
        slots_kernel,
        in_specs=[pl.BlockSpec(memory_space=pltpu.VMEM)] * 5,
        out_specs=pl.BlockSpec(memory_space=pltpu.HBM),
        out_shape=pltpu.HBM((16, *ahead[0].shape), ahead[0].dtype),
        scratch_shapes=[pltpu.SemaphoreType.DMA((16,))],
        cost_estimate=pl.CostEstimate(
            flops=16 * ahead[0].size, bytes_accessed=42 * ahead[0].size, transcendentals=0
        ),
        compiler_params=pltpu.CompilerParams(vmem_limit_bytes=SLOTS_VMEM),
        name="slots",
    )(*ahead)


def tile_kernel(place, left_ref, right_ref, *refs):
    out_ref, rows_ref, sems = refs[-3:]
    scale = 1.0 / right_ref.shape[0]
    copies = []
    for i, (start, size) in enumerate(PIECES):
        at = pl.ds(start, size)
        left = left_ref[start : start + size, :]
        product = jnp.dot(left, right_ref[...], preferred_element_type=jnp.float32)
        rows_ref[at, :] = product * scale
        copies.append(
            pltpu.make_async_copy(rows_ref.at[at], out_ref.at[place, at], sems.at[i])
        )
        copies[-1].start()
    for copy in copies:
        copy.wait()


def tile_into(place, keys_t, partner, tiles=None):
    width, count = keys_t.shape
    in_specs = [pl.BlockSpec(memory_space=pltpu.VMEM)] * 2
    args = [keys_t, partner]
    if tiles is not None:
        in_specs.append(pl.BlockSpec(memory_space=pltpu.HBM))
        args.append(tiles)
    return pl.pallas_call(
        functools.partial(tile_kernel, place),
        in_specs=in_specs,
        out_specs=pl.BlockSpec(memory_space=pltpu.HBM),
        out_shape=pltpu.HBM((2, width, width), jnp.float32),
        scratch_shapes=[
            pltpu.VMEM((width, width), jnp.float32),
            pltpu.SemaphoreType.DMA((len(PIECES),)),
        ],
        input_output_aliases={} if tiles is None else {2: 0},
        cost_estimate=pl.CostEstimate(
            flops=2 * width * width * count,
            bytes_accessed=4 * width * count + 4 * width * width,
            transcendentals=0,
        ),
        compiler_params=pltpu.CompilerParams(vmem_limit_bytes=TILE_VMEM),
        name="tile",
    )(*args)


def fetch_kernel(states_in, gate_in, up_in, squares_ref, states_ref, gate_ref, up_ref, sems):
    pairs = ((states_in, states_ref), (gate_in, gate_ref), (up_in, up_ref))
    copies = [pltpu.make_async_copy(a, b, sems.at[i]) for i, (a, b) in enumerate(pairs)]
    for copy in copies:
        copy.start()
    copies[0].wait()
    wide = states_ref[...].astype(jnp.float32)
    total = jnp.sum(wide * wide, axis=1, keepdims=True)
    total = jnp.broadcast_to(total, (wide.shape[0], 128)).T
    squares_ref[...] = jnp.broadcast_to(total[None, :1], squares_ref.shape)
    for copy in copies[1:]:
        copy.wait()


def fetched(states, gate_weight, up_weight, copies):
    arrays = (states, gate_weight, up_weight)
    count, depth = states.shape
    return pl.pallas_call(
        fetch_kernel,
        in_specs=[pl.BlockSpec(memory_space=pltpu.HBM)] * 3,
        out_specs=[pl.BlockSpec(memory_space=pltpu.VMEM)] * 4,
        out_shape=[pltpu.VMEM((copies, 1, count), jnp.float32)]
        + [pltpu.VMEM(array.shape, array.dtype) for array in arrays],
        scratch_shapes=[pltpu.SemaphoreType.DMA((3,))],
        cost_estimate=pl.CostEstimate(
            flops=2 * count * depth,
            bytes_accessed=2 * sum(array.size for array in arrays),
            transcendentals=0,
        ),
        compiler_params=pltpu.CompilerParams(vmem_limit_bytes=58 * 2**20),
        name="fetch",
    )(*arrays)


def sums_kernel(states_ref, squares_ref, gain_ref, gate_ref, up_ref, out_ref):
    width = gate_ref.shape[1]
    squares = jnp.sum(squares_ref[...], axis=0)
    inverse = lax.rsqrt(squares / D + 1e-05)
    inverse = jnp.broadcast_to(inverse, (128, inverse.shape[1])).T[:, :1]
    rows = states_ref.shape[0] // 2
    for i in range(2):
        at = slice(i * rows, (i + 1) * rows)
        normed = states_ref[at, :].astype(jnp.float32) * inverse[at, :] * gain_ref[...]
        normed = normed.astype(jnp.bfloat16)
        for j, weight in enumerate((gate_ref, up_ref)):
            part = jnp.dot(normed, weight[...], preferred_element_type=jnp.float32)
            out_ref[at, j * width : (j + 1) * width] = part.astype(jnp.bfloat16)


def partial_sums(states, squares, norm_gain, gate_weight, up_weight):
    count, depth = states.shape
    width = gate_weight.shape[1]
    return pl.pallas_call(
        sums_kernel,
        in_specs=[pl.BlockSpec(memory_space=pltpu.VMEM)] * 5,
        out_specs=pl.BlockSpec(memory_space=pltpu.VMEM),
        out_shape=jax.ShapeDtypeStruct((count, 2 * width), jnp.bfloat16),
        cost_estimate=pl.CostEstimate(
            flops=4 * count * depth * width,
            bytes_accessed=2 * (count * depth + 2 * depth * width + 2 * count * width),
            transcendentals=0,
        ),
        compiler_params=pltpu.CompilerParams(vmem_limit_bytes=24 * 2**20),
        name="sums",
    )(states, squares, norm_gain[None, :], gate_weight, up_weight)


def on_device(states, norm_gain, gate_weight, up_weight):
    n_col = lax.axis_size(COL)
    column = lax.axis_index(COL)
    yh, yl, core = lax.axis_index("yh"), lax.axis_index("yl"), lax.axis_index("k")
    count = states.shape[0]
    width = gate_weight.shape[1]
    share = count // n_col
    scale = 1.0 / count

    squares, *arrays = fetched(states, gate_weight, up_weight, n_col)
    parts = partial_sums(arrays[0], exchange(squares, COL), norm_gain, *arrays[1:])
    parts = exchange(parts.reshape(n_col, share, 2 * width), COL)
    summed = jnp.sum(parts.astype(jnp.float32), axis=0)
    own = (jax.nn.silu(summed[:, :width]) * summed[:, width:]).astype(jnp.bfloat16)

    ahead = [own]
    two = passed_along(own, "z", -2)
    one = passed_along(two, "z", 1)
    three = passed_along(two, "z", -1)
    keys = copy_for_each(own, COL).reshape(count, width)
    ahead = [own, one, two, three, passed_along(three, "z", -1)]
    outgoing, keys = lax.optimization_barrier((slots(ahead), keys))
    returned = exchange(outgoing, PLANE)

    slab = width // n_col
    own_cols = lax.dynamic_slice_in_dim(keys, column * slab, slab, 1)
    their_cols = passed_along(own_cols, "z", 4)
    their_far = (cross(their_cols, keys) * scale).astype(jnp.bfloat16)
    far_tiles = passed_along(their_far, "z", 4).astype(jnp.float32)[None]
    returned, far_tiles, keys_t = lax.optimization_barrier((returned, far_tiles, keys.T))

    returned = returned.reshape(4, 2, 2, share, width)
    near = jnp.bitwise_xor(yh, yl)
    swap = jnp.where(core == 0, 1 - near, near)
    second = lax.dynamic_index_in_dim(returned, swap, 1, keepdims=False)
    second = passed_along(second.reshape(count, width), "k", 1)
    first = lax.dynamic_index_in_dim(returned, near, 1, keepdims=False)
    tiles = tile_into(0, keys_t, first.reshape(count, width))
    near_tiles = tile_into(1, keys_t, second, tiles)[None]
    return (near_tiles, far_tiles)


def solution(mesh):
    torus = Mesh(mesh.devices.reshape(8, 2, 2, 4, 2), ("z", "yh", "k", "x", "yl"))
    in_specs = (P(None, COL), P(COL), P(COL, ROW), P(COL, ROW))
    out_specs = (P(ROW, COL, None, None), P(ROW, COL, None))

    return jax.shard_map(
        on_device, mesh=torus, in_specs=in_specs, out_specs=out_specs, check_vma=False
    )
```
